256 devices in a mesh: wide: 16 (over y_lo, x, core), narrow: 16 (over z, y_hi).
Axes of the slice: x: 4, y: 4 (y_hi: 2, y_lo: 2; y = y_hi * 2 + y_lo), z: 8, core: 2. Of those that a mesh axis runs over, the one named last changes fastest.
Arguments:
- right_side: bfloat16 [393216, 256], P(('wide', 'narrow')), may hold values from -6 to 6
- leaf_blocks: bfloat16 [393216, 1536], P(('wide', 'narrow')), may hold values from -8 to 16
- level_bases: bfloat16 [393216, 1024], P(('wide', 'narrow')), may hold values from -2 to 2
Outputs:
- solution_field: float32 [393216, 256], P(('wide', 'narrow'))
- residual: float32 [393216, 256], P(('wide', 'narrow'))
The draws below stay inside these ranges and needn't reach their ends.
All inputs are finite; a program needn't handle non-finite values.
Results may differ from the reference program's by a relative error of at most 0.006.
Values may be sent and summed in bfloat16 or wider, within the bound.
A program may use at most 64 MiB of HBM per device.

```python
import jax
import jax.numpy as jnp
from jax import lax

LEAF = 1536
RANK = 128
VECS = 256
ITERS = 2
LEVELS = 8
ORDER = 393216


def draw_leaf_blocks(key, part):
    blocks = ORDER // LEAF

    def one_block(index):
        subkey = jax.random.fold_in(key, index)
        first_key, second_key = jax.random.split(subkey, 2)
        noise = jnp.clip(jax.random.normal(first_key, (LEAF, LEAF), jnp.float32), -6.0, 6.0)
        symmetric = (noise + noise.T) * 0.5 ** 0.5 / LEAF ** 0.5
        diagonal = jax.random.uniform(second_key, (LEAF,), jnp.float32, 5.0, 7.0)
        return (symmetric + jnp.diag(diagonal)).astype(jnp.bfloat16)
    stacked = lax.map(one_block, jnp.arange(blocks))
    return stacked.reshape(ORDER, LEAF)


def draw_level_bases(key, part):
    scales = []
    for level_index in range(LEVELS):
        member = 2.0 ** level_index
        weight = 0.55
        scales.append(weight ** 0.5 * (LEAF * member * RANK) ** (-0.25))
    column_scale = jnp.repeat(jnp.array(scales, jnp.float32), RANK)
    first_key = jax.random.fold_in(jax.random.fold_in(key, 7), 0)
    noise = jnp.clip(jax.random.normal(first_key, (ORDER, LEVELS * RANK), jnp.float32), -6.0, 6.0)
    return (noise * column_scale[None, :]).astype(jnp.bfloat16)


def levels(stream_key, extent, shards, smallest, high):
    factor_of, own = 1.0, jax.random.fold_in(stream_key, 6)
    for dim, shards_of in shards:
        draws = jnp.exp(jax.random.uniform(jax.random.fold_in(own, dim), (shards_of,), jnp.float32, smallest / len(shards), high / len(shards)))
        factor_of = factor_of * jnp.repeat(draws, extent[dim] // shards_of).reshape([-1 if axis == dim else 1 for axis in range(len(extent))])
    return factor_of


def centred(stream_key, dims, scale, most, shards=(), kind=jnp.bfloat16):
    drawn = jax.random.normal(stream_key, dims, jnp.float32) * scale
    if len(shards) > 0:
        drawn = levels(stream_key, dims, shards, -0.22, 0.18) * drawn
    return jnp.clip(drawn, min=-most, max=most).astype(kind)


def setup_inputs(seed: int = 0) -> dict:
    key_list = jax.random.split(jax.random.key(seed), 4)
    return {
        "right_side": centred(key_list[0], (ORDER, VECS), 1.0, 6.0, ((0, 256),)),
        "leaf_blocks": draw_leaf_blocks(jax.random.fold_in(key_list[3], 71), 0),
        "level_bases": draw_level_bases(jax.random.fold_in(key_list[3], 71), 0),
    }


centre = 6.0
half_width = 5.0


def leaf_product(operands):
    return jnp.dot(operands[0], operands[1], preferred_element_type=jnp.float32)


def project_block(operands):
    return lax.dot_general(operands[1], operands[0], (((0,), (0,)), ((), ())), preferred_element_type=jnp.float32)


def expand_block(operands):
    return lax.dot_general(operands[0], operands[1], (((1,), (1,)), ((), ())), preferred_element_type=jnp.float32)


def apply_kernel(operand, leaf_blocks, level_bases):
    blocks = ORDER // LEAF
    leaf_three = leaf_blocks.reshape(blocks, LEAF, LEAF)
    operand_three = operand.reshape(blocks, LEAF, VECS)
    basis_three = level_bases.reshape(blocks, LEAF, LEVELS * RANK)
    leaf_part = lax.map(leaf_product, (leaf_three, operand_three))
    projected = lax.map(project_block, (basis_three, operand_three))
    siblings = []
    for level_index in range(LEVELS):
        member = 2 ** level_index
        columns = projected[:, :, level_index * RANK:(level_index + 1) * RANK]
        node_sums = columns.reshape(blocks // member, member, VECS, RANK).sum(axis=1)
        swapped = node_sums.reshape(blocks // (2 * member), 2, VECS, RANK)[:, ::-1]
        spread = jnp.broadcast_to(swapped.reshape(blocks // member, 1, VECS, RANK), (blocks // member, member, VECS, RANK))
        siblings.append(spread.reshape(blocks, VECS, RANK))
    stacked = jnp.concatenate(siblings, axis=2).astype(jnp.bfloat16)
    expanded = lax.map(expand_block, (basis_three, stacked))
    return (leaf_part + expanded).reshape(ORDER, VECS)


def reference(right_side, leaf_blocks, level_bases):
    residual = right_side.astype(jnp.float32)
    solution_field = jnp.zeros_like(residual, dtype=jnp.float32)
    sigma_ratio = centre / half_width
    ratio_now = 1.0 / sigma_ratio
    direction = residual / centre
    for iteration in range(ITERS):
        solution_field = solution_field + direction
        applied = apply_kernel(direction.astype(jnp.bfloat16), leaf_blocks, level_bases)
        residual = residual - applied
        if iteration + 1 < ITERS:
            ratio_next = 1.0 / (2.0 * sigma_ratio - ratio_now)
            direction = ratio_next * ratio_now * direction + (2.0 * ratio_next / half_width) * residual
            ratio_now = ratio_next
    return solution_field, residual
```

```python
import jax
import jax.numpy as jnp
from jax import lax
from jax.experimental import pallas as pl
from jax.experimental.pallas import tpu as pltpu
from jax.sharding import PartitionSpec as P

MESH = pl.DeviceIdType.MESH
F32, BF16 = jnp.float32, jnp.bfloat16
LEAF, RANK, VECS, LEVELS, ITERS = 1536, 128, 256, 8, 2
CENTRE, HALF = 6.0, 5.0
CH = 256
NCH = LEAF // CH
SIGMA = CENTRE / HALF
Q0 = 1.0 / SIGMA
Q1 = 1.0 / (2.0 * SIGMA - Q0)
KEEP, GAIN = Q1 * Q0, 2.0 * Q1 / HALF
S0, S1, S2, S3, SH, R1, R2, R3, RH, WH = range(10)


def flip(v, bit):
    return v + bit - 2 * bit * ((v // bit) % 2)


def kernel(
    r_hbm, l_hbm, b_hbm, x_hbm, o_hbm,
    r_v, l_v, b_v, d_v, acc_v, x_v, pacc, proj, sib, st,
    r1, r2, r3, rh, q1, q2, q3, qh, wv, tv,
    in_sem, out_sem, send_sem, recv_sem,
):
    w = lax.axis_index("wide")
    n = lax.axis_index("narrow")
    yl, x, c = w // 8, (w // 2) % 4, w % 2
    z, yh = n // 2, n % 2
    oyl = 1 - yl

    def dev(yl_, x_, c_, z_, yh_):
        return {"wide": yl_ * 8 + x_ * 2 + c_, "narrow": z_ * 2 + yh_}

    def rows(i, size):
        return pl.ds(pl.multiple_of(i * size, size), size)

    def send(src, dst, t, group, to):
        pltpu.make_async_remote_copy(
            src_ref=src, dst_ref=dst, send_sem=send_sem.at[t, group],
            recv_sem=recv_sem.at[t, group], device_id=to, device_id_type=MESH,
        ).start()

    def wait(ref, sem):
        pltpu.make_async_copy(ref, ref, sem).wait()

    pltpu.make_async_copy(r_hbm, r_v, in_sem.at[0]).start()
    for i in range(NCH):
        part = pl.ds(i * CH, CH)
        pltpu.make_async_copy(b_hbm.at[part], b_v.at[part], in_sem.at[1 + i]).start()
    for i in range(NCH):
        part = pl.ds(i * CH, CH)
        pltpu.make_async_copy(l_hbm.at[part], l_v.at[part], in_sem.at[1 + NCH + i]).start()

    barrier = pltpu.get_barrier_semaphore()

    def greet(to):
        pl.semaphore_signal(barrier, inc=1, device_id=to, device_id_type=MESH)

    def greet_ring(i, carry):
        for h in range(2):
            greet(dev(oyl, x, c, i, h))
        return carry

    lax.fori_loop(0, 8, greet_ring, 0)
    greet(dev(yl, x, c, z, 1 - yh))
    greet(dev(yl, x, 1 - c, z, yh))
    for dx in range(1, 4):
        for cc in range(2):
            greet(dev(yl, (x + dx) % 4, cc, z, yh))
    for dx in range(1, 4):
        for cc in range(2):
            greet(dev(oyl, (x + dx) % 4, cc, z, yh))
    greet(dev(oyl, x, 1 - c, z, yh))

    def project(k, first):
        part = rows(k, CH)
        p = lax.dot_general(
            d_v[part, :], b_v[part, :], (((0,), (0,)), ((), ())),
            preferred_element_type=F32,
        )
        if first:
            pacc[...] = p
        else:
            pacc[...] += p

    def scatter(t):
        for k in range(LEVELS):
            proj[t, k] = pacc[:, k * RANK:(k + 1) * RANK].astype(BF16)
        if t == 0:
            pl.semaphore_wait(barrier, 31)

        def ring(i, carry):
            step = jnp.where(i == 7, 0, jnp.where(i % 2 == 0, 4 + i // 2, 3 - i // 2))
            zz = (z + step) % 8
            for h in range(2):
                hh = (yh + 1 - h) % 2
                send(
                    proj.at[t, pl.ds(4, 4), rows(zz * 2 + hh, 16)], rh.at[t, n],
                    t, RH, dev(oyl, x, c, zz, hh),
                )
            return carry

        lax.fori_loop(0, 8, ring, 0)
        for a in range(4):
            zz = (z // 4) * 4 + (z % 4 + 3 - a + 4) % 4
            for h in range(2):
                send(
                    proj.at[t, 3, rows((zz % 4) * 2 + h, 32)],
                    r3.at[t, (z % 4) * 2 + yh], t, R3, dev(oyl, x, c, zz, h),
                )
        for a in range(2):
            zz = (z // 2) * 2 + (z % 2 + 1 - a) % 2
            for h in range(2):
                send(
                    proj.at[t, 2, rows((zz % 2) * 2 + h, 64)],
                    r2.at[t, (z % 2) * 2 + yh], t, R2, dev(oyl, x, c, zz, h),
                )
        for h in range(2):
            send(proj.at[t, 1, pl.ds(h * 128, 128)], r1.at[t, yh], t, R1, dev(oyl, x, c, z, h))
        send(proj.at[t, 0], sib.at[t, 0], t, S0, dev(yl, x, c, z, 1 - yh))

    def high_wide(t):
        wait(rh.at[t], recv_sem.at[t, RH])
        for k in range(4):
            total = rh[t, 0, k].astype(F32)
            for i in range(1, 16):
                total = total + rh[t, i, k].astype(F32)
            qh[t, k] = total.astype(BF16)
        for dx in range(3, -1, -1):
            for cc in range(2):
                send(qh.at[t, 3], wv.at[t, 7 + x * 2 + c], t, WH, dev(oyl, (x + dx) % 4, cc, z, yh))
        for a in range(2):
            xx = (flip(x, 2) // 2) * 2 + a
            for cc in range(2):
                send(qh.at[t, 2], wv.at[t, 3 + (x % 2) * 2 + c], t, WH, dev(yl, xx, cc, z, yh))
        for cc in range(2):
            send(qh.at[t, 1], wv.at[t, 1 + c], t, WH, dev(yl, flip(x, 1), cc, z, yh))
        send(qh.at[t, 0], wv.at[t, 0], t, WH, dev(yl, x, 1 - c, z, yh))

    def high_spread(t):
        wait(wv.at[t], recv_sem.at[t, WH])
        tv[t, 0] = wv[t, 0]
        tv[t, 1] = (wv[t, 1].astype(F32) + wv[t, 2].astype(F32)).astype(BF16)
        total = wv[t, 3].astype(F32)
        for i in range(4, 7):
            total = total + wv[t, i].astype(F32)
        tv[t, 2] = total.astype(BF16)
        total = wv[t, 7].astype(F32)
        for i in range(8, 15):
            total = total + wv[t, i].astype(F32)
        tv[t, 3] = total.astype(BF16)

        def ring(i, carry):
            step = jnp.where(i == 7, 0, jnp.where(i % 2 == 0, 4 + i // 2, 3 - i // 2))
            zz = (z + step) % 8
            for h in range(2):
                send(
                    tv.at[t], sib.at[t, pl.ds(4, 4), rows(n, 16)],
                    t, SH, dev(oyl, x, c, zz, h),
                )
            return carry

        lax.fori_loop(0, 8, ring, 0)

    def low(t):
        wait(r1.at[t], recv_sem.at[t, R1])
        q1[t] = (r1[t, 0].astype(F32) + r1[t, 1].astype(F32)).astype(BF16)
        for h in range(2):
            send(q1.at[t], sib.at[t, 1, rows(yh, 128)], t, S1, dev(oyl, x, c, flip(z, 1), h))
        wait(r2.at[t], recv_sem.at[t, R2])
        total = r2[t, 0].astype(F32)
        for i in range(1, 4):
            total = total + r2[t, i].astype(F32)
        q2[t] = total.astype(BF16)
        for a in range(2):
            zz = (flip(z, 2) // 2) * 2 + a
            for h in range(2):
                send(q2.at[t], sib.at[t, 2, rows((z % 2) * 2 + yh, 64)], t, S2, dev(oyl, x, c, zz, h))
        wait(r3.at[t], recv_sem.at[t, R3])
        total = r3[t, 0].astype(F32)
        for i in range(1, 8):
            total = total + r3[t, i].astype(F32)
        q3[t] = total.astype(BF16)
        for a in range(4):
            zz = (1 - z // 4) * 4 + a
            for h in range(2):
                send(q3.at[t], sib.at[t, 3, rows((z % 4) * 2 + yh, 32)], t, S3, dev(oyl, x, c, zz, h))

    def leaf(k, load):
        part = rows(k, CH)
        return jnp.dot(l_v[part, :], d_v[...], preferred_element_type=F32)

    wait(r_v, in_sem.at[0])
    d_v[...] = (r_v[...].astype(F32) / CENTRE).astype(BF16)
    for k in range(NCH):
        part = pl.ds(k * CH, CH)
        wait(b_v.at[part], in_sem.at[1 + k])
        project(k, k == 0)
    scatter(0)
    for k in range(NCH):
        part = pl.ds(k * CH, CH)
        wait(l_v.at[part], in_sem.at[1 + NCH + k])

    def leaf_0(k, carry):
        part = rows(k, CH)
        acc_v[part, :] = r_v[part, :].astype(F32) - leaf(k, True)
        return carry

    lax.fori_loop(0, NCH, leaf_0, 0)
    high_wide(0)
    low(0)
    high_spread(0)

    def gather_low(t):
        for k, s in ((0, S0), (1, S1), (2, S2), (3, S3)):
            wait(sib.at[t, k], recv_sem.at[t, s])
            st[k * RANK:(k + 1) * RANK, :] = sib[t, k].T

    def gather_high(t):
        wait(sib.at[t, pl.ds(4, 4)], recv_sem.at[t, SH])
        for k in range(4, LEVELS):
            st[k * RANK:(k + 1) * RANK, :] = sib[t, k].T

    def expand_low(k, carry):
        part = rows(k, CH)
        acc_v[part, :] -= jnp.dot(
            b_v[part, 0:4 * RANK], st[0:4 * RANK, :], preferred_element_type=F32
        )
        return carry

    def expand_high(k):
        part = rows(k, CH)
        return acc_v[part, :] - jnp.dot(
            b_v[part, 4 * RANK:], st[4 * RANK:, :], preferred_element_type=F32
        )

    gather_low(0)
    lax.fori_loop(0, NCH, expand_low, 0)
    gather_high(0)
    pacc[...] = jnp.zeros_like(pacc)

    def middle(k, carry):
        part = rows(k, CH)
        residual = expand_high(k)
        d0 = r_v[part, :].astype(F32) / CENTRE
        d1 = KEEP * d0 + GAIN * residual
        acc_v[part, :] = residual
        x_v[part, :] = d0 + d1
        d_v[part, :] = d1.astype(BF16)
        project(k, False)
        return carry

    lax.fori_loop(0, NCH, middle, 0)
    scatter(1)
    pltpu.make_async_copy(x_v, x_hbm, out_sem.at[0]).start()

    def leaf_1(k, carry):
        part = rows(k, CH)
        acc_v[part, :] -= leaf(k, False)
        return carry

    lax.fori_loop(0, NCH, leaf_1, 0)
    high_wide(1)
    low(1)
    high_spread(1)
    gather_low(1)
    lax.fori_loop(0, NCH, expand_low, 0)
    gather_high(1)
    for k in range(NCH):
        part = pl.ds(k * CH, CH)
        acc_v[part, :] = expand_high(k)
        pltpu.make_async_copy(acc_v.at[part], o_hbm.at[part], out_sem.at[1 + k]).start()

    for t in range(ITERS):
        for k, s in ((0, S0), (1, R1), (2, R2), (3, R3), (1, S1), (2, S2), (3, S3)):
            wait(proj.at[t, k], send_sem.at[t, s])
        for s in (RH, SH):
            wait(proj.at[t, pl.ds(4, 4)], send_sem.at[t, s])
        wait(wv.at[t], send_sem.at[t, WH])
    wait(x_v, out_sem.at[0])
    for k in range(NCH):
        part = pl.ds(k * CH, CH)
        wait(acc_v.at[part], out_sem.at[1 + k])


def on_device(right_side, leaf_blocks, level_bases):
    any_space = pl.BlockSpec(memory_space=pl.ANY)
    out = jax.ShapeDtypeStruct((LEAF, VECS), F32)
    return pl.pallas_call(
        kernel,
        out_shape=(out, out),
        in_specs=[any_space] * 3,
        out_specs=(any_space, any_space),
        scratch_shapes=[
            pltpu.VMEM((LEAF, VECS), BF16),
            pltpu.VMEM((LEAF, LEAF), BF16),
            pltpu.VMEM((LEAF, LEVELS * RANK), BF16),
            pltpu.VMEM((LEAF, VECS), BF16),
            pltpu.VMEM((LEAF, VECS), F32),
            pltpu.VMEM((LEAF, VECS), F32),
            pltpu.VMEM((VECS, LEVELS * RANK), F32),
            pltpu.VMEM((ITERS, LEVELS, VECS, RANK), BF16),
            pltpu.VMEM((ITERS, LEVELS, VECS, RANK), BF16),
            pltpu.VMEM((LEVELS * RANK, VECS), BF16),
            pltpu.VMEM((ITERS, 2, 128, RANK), BF16),
            pltpu.VMEM((ITERS, 4, 64, RANK), BF16),
            pltpu.VMEM((ITERS, 8, 32, RANK), BF16),
            pltpu.VMEM((ITERS, 16, 4, 16, RANK), BF16),
            pltpu.VMEM((ITERS, 128, RANK), BF16),
            pltpu.VMEM((ITERS, 64, RANK), BF16),
            pltpu.VMEM((ITERS, 32, RANK), BF16),
            pltpu.VMEM((ITERS, 4, 16, RANK), BF16),
            pltpu.VMEM((ITERS, 15, 16, RANK), BF16),
            pltpu.VMEM((ITERS, 4, 16, RANK), BF16),
            pltpu.SemaphoreType.DMA((1 + 2 * NCH,)),
            pltpu.SemaphoreType.DMA((1 + NCH,)),
            pltpu.SemaphoreType.DMA((ITERS, 10)),
            pltpu.SemaphoreType.DMA((ITERS, 10)),
        ],
        compiler_params=pltpu.CompilerParams(
            collective_id=0, has_side_effects=True, vmem_limit_bytes=48 * 1024 * 1024
        ),
        name="chebyshev",
    )(right_side, leaf_blocks, level_bases)


def solution(mesh):
    return jax.shard_map(
        on_device,
        mesh=mesh,
        in_specs=(P(("wide", "narrow"), None),) * 3,
        out_specs=(P(("wide", "narrow"), None),) * 2,
        check_vma=False,
    )
```

```python
import jax
import jax.numpy as jnp
from jax import lax
from jax.experimental import pallas as pl
from jax.experimental.pallas import tpu as pltpu
from jax.sharding import PartitionSpec as P

MESH = pl.DeviceIdType.MESH
F32, BF16 = jnp.float32, jnp.bfloat16
LEAF, RANK, VECS, LEVELS, ITERS = 1536, 128, 256, 8, 2
COLS = LEVELS * RANK
HIGH = 4 * RANK
CENTRE, HALF = 6.0, 5.0
CH = 256
NCH = LEAF // CH
BIG = 512
NBIG = LEAF // BIG
SIGMA = CENTRE / HALF
Q0 = 1.0 / SIGMA
Q1 = 1.0 / (2.0 * SIGMA - Q0)
KEEP, GAIN = Q1 * Q0, 2.0 * Q1 / HALF
S0, S1, S2, S3, S4, S5, S67, R0, R1, R2, R3, RH, D5, P1, P6, P7 = range(16)
PEERS = 52


def flip(v, bit):
    return v + bit - 2 * bit * ((v // bit) % 2)


def kernel(
    r_hbm, l_hbm, b_hbm,
    acc_v, x_v, b_v, st,
    r_v, l_v, d_v, u_v, pacc, gacc, gram, proj, sib,
    r0, r1, r2, r3, rh, d5, p1, w6, w7, q1, q2, q3, q45, t4, t5, qp, tp,
    in_sem, send_sem, recv_sem,
):
    w = lax.axis_index("wide")
    n = lax.axis_index("narrow")
    yl, x, c = w // 8, (w // 2) % 4, w % 2
    z, yh = n // 2, n % 2
    oyl = 1 - yl
    plane = x * 4 + c * 2 + yh

    def dev(yl_, x_, c_, z_, yh_):
        return {"wide": yl_ * 8 + x_ * 2 + c_, "narrow": z_ * 2 + yh_}

    def rows(i, size):
        return pl.ds(pl.multiple_of(i * size, size), size)

    def send(src, dst, t, group, to):
        pltpu.make_async_remote_copy(
            src_ref=src, dst_ref=dst, send_sem=send_sem.at[t, group],
            recv_sem=recv_sem.at[t, group], device_id=to, device_id_type=MESH,
        ).start()

    def wait(ref, sem):
        pltpu.make_async_copy(ref, ref, sem).wait()

    def add(refs):
        total = refs[0].astype(F32)
        for ref in refs[1:]:
            total = total + ref.astype(F32)
        return total

    def far_first(i):
        return jnp.where(i == 7, 0, jnp.where(i % 2 == 0, 4 + i // 2, 3 - i // 2))

    barrier = pltpu.get_barrier_semaphore()

    def greet(to):
        pl.semaphore_signal(barrier, inc=1, device_id=to, device_id_type=MESH)

    def greet_ring(i, carry):
        zz = (z + far_first(i)) % 8
        for h in range(2):
            greet(dev(oyl, x, c, zz, h))
            greet(dev(oyl, flip(x, 1), c, zz, h))
        return carry

    pltpu.make_async_copy(r_hbm, r_v, in_sem.at[0]).start()
    for i in range(NCH):
        part = pl.ds(i * CH, CH)
        pltpu.make_async_copy(b_hbm.at[part], b_v.at[part], in_sem.at[1 + i]).start()
    for i in range(NCH):
        part = pl.ds(i * CH, CH)
        pltpu.make_async_copy(l_hbm.at[part], l_v.at[part], in_sem.at[1 + NCH + i]).start()

    lax.fori_loop(0, 8, greet_ring, 0)

    def greet_line(i, carry):
        greet(dev(yl, x, c, (z + 1 + i) % 8, yh))
        return carry

    lax.fori_loop(0, 7, greet_line, 0)
    for h in range(2):
        for cc in range(2):
            greet(dev(oyl, flip(x, 2), cc, z, h))
            greet(dev(oyl, flip(flip(x, 1), 2), cc, z, h))
        greet(dev(oyl, x, 1 - c, z, h))
        greet(dev(oyl, flip(x, 1), 1 - c, z, h))
    greet(dev(yl, x, 1 - c, z, yh))

    def contract(lhs, cols, total):
        def step(k, carry):
            part = rows(k, BIG)
            p = lax.dot_general(
                lhs[part, cols], b_v[part, :], (((0,), (0,)), ((), ())),
                preferred_element_type=F32,
            )
            total[...] = jnp.where(k == 0, p, total[...] + p)
            return carry

        lax.fori_loop(0, NBIG, step, 0)

    def scatter(t):
        def convert(k):
            proj[t, k] = pacc[:, k * RANK:(k + 1) * RANK].astype(BF16)

        convert(6)
        convert(7)
        if t == 0:
            for k in (5, 4, 3, 2, 1, 0):
                convert(k)
            pl.semaphore_wait(barrier, PEERS)

        def across(i, carry):
            xx = (x + 2 + i) % 4
            for cc in range(2):
                for h in range(2):
                    send(
                        proj.at[t, pl.ds(6, 2), rows(xx * 4 + cc * 2 + h, 16)], p1.at[t, plane],
                        t, P1, dev(oyl, xx, cc, z, h),
                    )
            return carry

        lax.fori_loop(0, 4, across, 0)
        if t > 0:
            convert(4)
            convert(5)

        def ring(i, carry):
            zz = (z + far_first(i)) % 8
            for h in range(2):
                send(
                    proj.at[t, pl.ds(4, 2), rows(zz * 2 + h, 16)], rh.at[t, n],
                    t, RH, dev(oyl, x, c, zz, h),
                )
            return carry

        lax.fori_loop(0, 8, ring, 0)
        if t > 0:
            for k in (3, 2, 1, 0):
                convert(k)
        for a in range(4):
            zz = (1 - z // 4) * 4 + (z + a) % 4
            for h in range(2):
                send(
                    proj.at[t, 3, rows((zz % 4) * 2 + h, 32)],
                    r3.at[t, (z % 4) * 2 + yh], t, R3, dev(oyl, x, c, zz, h),
                )
        for a in range(2):
            zz = (flip(z, 2) // 2) * 2 + (z + a) % 2
            for h in range(2):
                send(
                    proj.at[t, 2, rows((zz % 2) * 2 + h, 64)],
                    r2.at[t, (z % 2) * 2 + yh], t, R2, dev(oyl, x, c, zz, h),
                )
        for h in range(2):
            send(
                proj.at[t, 1, pl.ds(h * 128, 128)], r1.at[t, yh],
                t, R1, dev(oyl, x, c, flip(z, 1), h),
            )
        for h in range(2):
            send(proj.at[t, 0, pl.ds(h * 128, 128)], r0.at[t, yh], t, R0, dev(oyl, x, c, z, h))

    def own_plane(t):
        wait(p1.at[t], recv_sem.at[t, P1])
        qp[t, 0] = add([p1[t, i, 0] for i in range(8)]).astype(BF16)
        qp[t, 1] = add([p1[t, i, 0] for i in range(8, 16)]).astype(BF16)
        qp[t, 2] = add([p1[t, i, 1] for i in range(16)]).astype(BF16)

        def line(i, carry):
            dz = far_first(i)
            zz = (z + dz) % 8
            send(qp.at[t, pl.ds(0, 2)], w6.at[t, dz - 1], t, P6, dev(yl, x, c, zz, yh))
            send(qp.at[t, 2], w7.at[t, dz], t, P7, dev(oyl, x, c, zz, yh))
            return carry

        lax.fori_loop(0, 7, line, 0)
        send(qp.at[t, 2], w7.at[t, 0], t, P7, dev(oyl, x, c, z, yh))

    def own_line(t):
        wait(w6.at[t], recv_sem.at[t, P6])
        for j in range(2):
            tp[t, 1 - j, 0] = add([qp[t, j]] + [w6[t, i, j] for i in range(7)]).astype(BF16)
        wait(w7.at[t], recv_sem.at[t, P7])
        top = add([w7[t, i] for i in range(8)]).astype(BF16)
        tp[t, 0, 1] = top
        tp[t, 1, 1] = top

        def across(i, carry):
            xx = (x + 2 + i) % 4
            for cc in range(2):
                for h in range(2):
                    send(
                        tp.at[t, xx // 2], sib.at[t, pl.ds(6, 2), rows(plane, 16)],
                        t, S67, dev(oyl, xx, cc, z, h),
                    )
            return carry

        lax.fori_loop(0, 4, across, 0)

    def own_ring(t):
        wait(rh.at[t], recv_sem.at[t, RH])
        for k in range(2):
            q45[t, k] = add([rh[t, i, k] for i in range(16)])
        send(q45.at[t], d5.at[t], t, D5, dev(yl, x, 1 - c, z, yh))

    def own_pair(t):
        wait(d5.at[t], recv_sem.at[t, D5])
        t5[t] = (q45[t, 1] + d5[t, 1]).astype(BF16)
        t4[t] = d5[t, 0].astype(BF16)

        def ring(i, carry):
            zz = (z + far_first(i)) % 8
            for h in range(2):
                send(t5.at[t], sib.at[t, 5, rows(n, 16)], t, S5, dev(oyl, flip(x, 1), c, zz, h))
                send(t4.at[t], sib.at[t, 4, rows(n, 16)], t, S4, dev(oyl, x, c, zz, h))
            return carry

        lax.fori_loop(0, 8, ring, 0)

    def own_0(t):
        wait(r0.at[t], recv_sem.at[t, R0])
        for h in range(2):
            send(r0.at[t, 1 - h], sib.at[t, 0, rows(yh, 128)], t, S0, dev(oyl, x, c, z, h))

    def own_1(t):
        wait(r1.at[t], recv_sem.at[t, R1])
        q1[t] = add([r1[t, 0], r1[t, 1]]).astype(BF16)
        for h in range(2):
            send(q1.at[t], sib.at[t, 1, rows(yh, 128)], t, S1, dev(oyl, x, c, z, h))

    def own_2(t):
        wait(r2.at[t], recv_sem.at[t, R2])
        q2[t] = add([r2[t, i] for i in range(4)]).astype(BF16)
        for a in range(2):
            zz = (z // 2) * 2 + (z + 1 + a) % 2
            for h in range(2):
                send(q2.at[t], sib.at[t, 2, rows((z % 2) * 2 + yh, 64)], t, S2, dev(oyl, x, c, zz, h))

    def own_3(t):
        wait(r3.at[t], recv_sem.at[t, R3])
        q3[t] = add([r3[t, i] for i in range(8)]).astype(BF16)
        for a in range(4):
            zz = (z // 4) * 4 + (z + 2 + a) % 4
            for h in range(2):
                send(q3.at[t], sib.at[t, 3, rows((z % 4) * 2 + yh, 32)], t, S3, dev(oyl, x, c, zz, h))

    def arrive(t, groups):
        for k, count, s in groups:
            ref = sib.at[t, k] if count == 1 else sib.at[t, pl.ds(k, count)]
            wait(ref, recv_sem.at[t, s])

    def turn(t, levels):
        for k in levels:
            st[k * RANK:(k + 1) * RANK, :] = sib[t, k].T

    LOW = ((0, 1, S0), (1, 1, S1), (2, 1, S2), (3, 1, S3))

    def gram_block(i):
        contract(b_v, pl.ds(i * 256, 256), gacc)
        gram[pl.ds(i * 256, 256), :] = (GAIN * gacc[...]).astype(BF16)

    def through_gram(pair):
        both = jnp.concatenate([sib[0, 2 * pair], sib[0, 2 * pair + 1]], axis=1)
        pacc[...] -= jnp.dot(
            both, gram[pl.ds(pair * 256, 256), :], preferred_element_type=F32
        )

    wait(r_v, in_sem.at[0])
    d_v[...] = (r_v[...].astype(F32) / CENTRE).astype(BF16)
    for k in range(NCH):
        part = pl.ds(k * CH, CH)
        wait(b_v.at[part], in_sem.at[1 + k])
        p = lax.dot_general(
            d_v[part, :], b_v[part, :], (((0,), (0,)), ((), ())), preferred_element_type=F32
        )
        pacc[...] = p if k == 0 else pacc[...] + p
    scatter(0)
    for k in range(NCH):
        part = pl.ds(k * CH, CH)
        wait(l_v.at[part], in_sem.at[1 + NCH + k])

    def leaf_0(k, carry):
        part = rows(k, BIG)
        first = r_v[part, :].astype(F32)
        rest = first - jnp.dot(l_v[part, :], d_v[...], preferred_element_type=F32)
        acc_v[part, :] = rest
        u_v[part, :] = (KEEP * (first / CENTRE) + GAIN * rest).astype(BF16)
        return carry

    lax.fori_loop(0, NBIG, leaf_0, 0)
    contract(u_v, slice(None), pacc)
    gram_block(0)
    own_plane(0)
    own_ring(0)
    own_pair(0)
    own_3(0)
    own_2(0)
    own_1(0)
    own_0(0)
    gram_block(1)
    own_line(0)
    gram_block(2)
    gram_block(3)
    arrive(0, LOW)
    through_gram(0)
    through_gram(1)
    arrive(0, ((4, 1, S4), (5, 1, S5)))
    through_gram(2)
    arrive(0, ((6, 2, S67),))
    through_gram(3)
    scatter(1)

    turn(0, range(LEVELS))

    def middle(k, carry):
        part = rows(k, BIG)
        rest = acc_v[part, :] - jnp.dot(b_v[part, :], st[...], preferred_element_type=F32)
        d0 = r_v[part, :].astype(F32) / CENTRE
        d1 = KEEP * d0 + GAIN * rest
        acc_v[part, :] = rest
        x_v[part, :] = d0 + d1
        d_v[part, :] = d1.astype(BF16)
        return carry

    lax.fori_loop(0, NBIG, middle, 0)

    def leaf_1(k, carry):
        part = rows(k, BIG)
        acc_v[part, :] -= jnp.dot(l_v[part, :], d_v[...], preferred_element_type=F32)
        return carry

    lax.fori_loop(0, NBIG, leaf_1, 0)
    own_plane(1)
    own_ring(1)
    own_pair(1)
    own_3(1)
    own_2(1)
    own_1(1)
    own_0(1)
    own_line(1)
    arrive(1, LOW)
    turn(1, range(4))

    def expand_low(k, carry):
        part = rows(k, BIG)
        acc_v[part, :] -= jnp.dot(
            b_v[part, 0:HIGH], st[0:HIGH, :], preferred_element_type=F32
        )
        return carry

    lax.fori_loop(0, NBIG, expand_low, 0)

    for t in range(ITERS):
        for k, s in ((0, S0), (0, R0), (1, R1), (2, R2), (3, R3), (1, S1), (2, S2), (3, S3), (4, S4), (5, S5)):
            wait(proj.at[t, k], send_sem.at[t, s])
        wait(proj.at[t, pl.ds(4, 2)], send_sem.at[t, RH])
        wait(proj.at[t, pl.ds(6, 2)], send_sem.at[t, P1])
        wait(proj.at[t, pl.ds(6, 2)], send_sem.at[t, S67])
        wait(w6.at[t], send_sem.at[t, P6])
        wait(w7.at[t], send_sem.at[t, P7])
        wait(d5.at[t], send_sem.at[t, D5])
    arrive(1, ((4, 1, S4), (5, 1, S5)))
    turn(1, (4, 5))
    arrive(1, ((6, 2, S67),))
    turn(1, (6, 7))


def finish(acc_v, x_v, b_v, st, x_hbm, o_hbm, o_v, sem):
    copies = [pltpu.make_async_copy(x_v, x_hbm, sem.at[0])]
    copies[0].start()
    for k in range(NCH):
        part = pl.ds(k * CH, CH)
        o_v[part, :] = acc_v[part, :] - jnp.dot(
            b_v[part, HIGH:], st[HIGH:, :], preferred_element_type=F32
        )
        copies.append(pltpu.make_async_copy(o_v.at[part], o_hbm.at[part], sem.at[1 + k]))
        copies[-1].start()
    for copy in copies:
        copy.wait()


def on_device(right_side, leaf_blocks, level_bases):
    hbm = pl.BlockSpec(memory_space=pltpu.HBM)
    vmem = pl.BlockSpec(memory_space=pltpu.VMEM)
    field = jax.ShapeDtypeStruct((LEAF, VECS), F32)
    state = pl.pallas_call(
        kernel,
        out_shape=(
            field, field, jax.ShapeDtypeStruct((LEAF, COLS), BF16),
            jax.ShapeDtypeStruct((COLS, VECS), BF16),
        ),
        in_specs=[hbm] * 3,
        out_specs=(vmem,) * 4,
        scratch_shapes=[
            pltpu.VMEM((LEAF, VECS), BF16),
            pltpu.VMEM((LEAF, LEAF), BF16),
            pltpu.VMEM((LEAF, VECS), BF16),
            pltpu.VMEM((LEAF, VECS), BF16),
            pltpu.VMEM((VECS, COLS), F32),
            pltpu.VMEM((VECS, COLS), F32),
            pltpu.VMEM((COLS, COLS), BF16),
            pltpu.VMEM((ITERS, LEVELS, VECS, RANK), BF16),
            pltpu.VMEM((ITERS, LEVELS, VECS, RANK), BF16),
            pltpu.VMEM((ITERS, 2, 128, RANK), BF16),
            pltpu.VMEM((ITERS, 2, 128, RANK), BF16),
            pltpu.VMEM((ITERS, 4, 64, RANK), BF16),
            pltpu.VMEM((ITERS, 8, 32, RANK), BF16),
            pltpu.VMEM((ITERS, 16, 2, 16, RANK), BF16),
            pltpu.VMEM((ITERS, 2, 16, RANK), F32),
            pltpu.VMEM((ITERS, 16, 2, 16, RANK), BF16),
            pltpu.VMEM((ITERS, 7, 2, 16, RANK), BF16),
            pltpu.VMEM((ITERS, 8, 16, RANK), BF16),
            pltpu.VMEM((ITERS, 128, RANK), BF16),
            pltpu.VMEM((ITERS, 64, RANK), BF16),
            pltpu.VMEM((ITERS, 32, RANK), BF16),
            pltpu.VMEM((ITERS, 2, 16, RANK), F32),
            pltpu.VMEM((ITERS, 16, RANK), BF16),
            pltpu.VMEM((ITERS, 16, RANK), BF16),
            pltpu.VMEM((ITERS, 3, 16, RANK), BF16),
            pltpu.VMEM((ITERS, 2, 2, 16, RANK), BF16),
            pltpu.SemaphoreType.DMA((1 + 2 * NCH,)),
            pltpu.SemaphoreType.DMA((ITERS, 16)),
            pltpu.SemaphoreType.DMA((ITERS, 16)),
        ],
        compiler_params=pltpu.CompilerParams(
            collective_id=0, has_side_effects=True, vmem_limit_bytes=40 * 1024 * 1024
        ),
        name="chebyshev",
    )(*(pltpu.with_memory_space_constraint(v, pltpu.HBM) for v in (right_side, leaf_blocks, level_bases)))
    return pl.pallas_call(
        finish,
        out_shape=(field, field),
        in_specs=[vmem] * 4,
        out_specs=(hbm, hbm),
        scratch_shapes=[
            pltpu.VMEM((LEAF, VECS), F32),
            pltpu.SemaphoreType.DMA((1 + NCH,)),
        ],
        compiler_params=pltpu.CompilerParams(vmem_limit_bytes=16 * 1024 * 1024),
        name="finish",
    )(*state)


def solution(mesh):
    return jax.shard_map(
        on_device,
        mesh=mesh,
        in_specs=(P(("wide", "narrow"), None),) * 3,
        out_specs=(P(("wide", "narrow"), None),) * 2,
        check_vma=False,
    )
```

```python
import jax
import jax.numpy as jnp
from jax import lax
from jax.experimental import pallas as pl
from jax.experimental.pallas import tpu as pltpu
from jax.sharding import PartitionSpec as P

MESH = pl.DeviceIdType.MESH
F32, BF16 = jnp.float32, jnp.bfloat16
LEAF, RANK, VECS, LEVELS, ITERS = 1536, 128, 256, 8, 2
COLS = LEVELS * RANK
HIGH = 4 * RANK
CENTRE, HALF = 6.0, 5.0
CH = 256
NCH = LEAF // CH
BIG = 512
NBIG = LEAF // BIG
SIGMA = CENTRE / HALF
Q0 = 1.0 / SIGMA
Q1 = 1.0 / (2.0 * SIGMA - Q0)
KEEP, GAIN = Q1 * Q0, 2.0 * Q1 / HALF
S0, S1, S2, S3, S4, S5, S67, R0, R1, R2, R3, RH, D5, F5, P1, P6, P7 = range(17)
PEERS = 52


def flip(v, bit):
    return v + bit - 2 * bit * ((v // bit) % 2)


def kernel(
    r_hbm, l_hbm, b_hbm,
    acc_v, x_v, b_v, st,
    r_v, l_v, d_v, u_v, pacc, gacc, gram, proj, sib,
    r0, r1, r2, r3, rh, d5, p1, w6, w7, q1, q2, q3, q45, t4, t5, qp, tp,
    in_sem, send_sem, recv_sem,
):
    w = lax.axis_index("wide")
    n = lax.axis_index("narrow")
    yl, x, c = w // 8, (w // 2) % 4, w % 2
    z, yh = n // 2, n % 2
    oyl = 1 - yl
    plane = x * 4 + c * 2 + yh

    def dev(yl_, x_, c_, z_, yh_):
        return {"wide": yl_ * 8 + x_ * 2 + c_, "narrow": z_ * 2 + yh_}

    def rows(i, size):
        return pl.ds(pl.multiple_of(i * size, size), size)

    def send(src, dst, t, group, to):
        pltpu.make_async_remote_copy(
            src_ref=src, dst_ref=dst, send_sem=send_sem.at[t, group],
            recv_sem=recv_sem.at[t, group], device_id=to, device_id_type=MESH,
        ).start()

    def wait(ref, sem):
        pltpu.make_async_copy(ref, ref, sem).wait()

    def add(refs):
        total = refs[0].astype(F32)
        for ref in refs[1:]:
            total = total + ref.astype(F32)
        return total

    def far_first(i):
        return jnp.where(i == 7, 0, jnp.where(i % 2 == 0, 4 + i // 2, 3 - i // 2))

    barrier = pltpu.get_barrier_semaphore()

    def greet(to):
        pl.semaphore_signal(barrier, inc=1, device_id=to, device_id_type=MESH)

    def greet_ring(i, carry):
        zz = (z + far_first(i)) % 8
        for h in range(2):
            greet(dev(oyl, x, c, zz, h))
            greet(dev(oyl, flip(x, 1), c, zz, h))
        return carry

    pltpu.make_async_copy(r_hbm, r_v, in_sem.at[0]).start()

    def load_bases(side):
        cols = pl.ds((1 - side) * HIGH, HIGH)
        for i in range(NCH):
            part = pl.ds(i * CH, CH)
            pltpu.make_async_copy(
                b_hbm.at[part, cols], b_v.at[part, cols], in_sem.at[1 + side * NCH + i]
            ).start()

    load_bases(0)
    lax.fori_loop(0, 8, greet_ring, 0)

    def greet_line(i, carry):
        greet(dev(yl, x, c, (z + 1 + i) % 8, yh))
        return carry

    lax.fori_loop(0, 7, greet_line, 0)
    for h in range(2):
        for cc in range(2):
            greet(dev(oyl, flip(x, 2), cc, z, h))
            greet(dev(oyl, flip(flip(x, 1), 2), cc, z, h))
        greet(dev(oyl, x, 1 - c, z, h))
        greet(dev(oyl, flip(x, 1), 1 - c, z, h))
    greet(dev(yl, x, 1 - c, z, yh))
    load_bases(1)
    for i in range(NCH):
        part = pl.ds(i * CH, CH)
        pltpu.make_async_copy(l_hbm.at[part], l_v.at[part], in_sem.at[1 + 2 * NCH + i]).start()

    def contract(lhs, cols, total):
        def step(k, carry):
            part = rows(k, BIG)
            p = lax.dot_general(
                lhs[part, cols], b_v[part, :], (((0,), (0,)), ((), ())),
                preferred_element_type=F32,
            )
            total[...] = jnp.where(k == 0, p, total[...] + p)
            return carry

        lax.fori_loop(0, NBIG, step, 0)

    def convert(t, levels):
        for k in levels:
            proj[t, k] = pacc[:, k * RANK:(k + 1) * RANK].astype(BF16)

    def scatter_67(t):
        def across(i, carry):
            xx = (x + 2 + i) % 4
            for cc in range(2):
                for h in range(2):
                    send(
                        proj.at[t, pl.ds(6, 2), rows(xx * 4 + cc * 2 + h, 16)], p1.at[t, plane],
                        t, P1, dev(oyl, xx, cc, z, h),
                    )
            return carry

        lax.fori_loop(0, 4, across, 0)

    def scatter_45(t):
        def ring(i, carry):
            zz = (z + far_first(i)) % 8
            for h in range(2):
                send(
                    proj.at[t, pl.ds(4, 2), rows(h * 8 + zz, 16)], rh.at[t, n],
                    t, RH, dev(oyl, x, c, zz, h),
                )
            return carry

        lax.fori_loop(0, 8, ring, 0)

    def scatter_3(t):
        for a in range(4):
            zz = (1 - z // 4) * 4 + (z + a) % 4
            for h in range(2):
                send(
                    proj.at[t, 3, rows((zz % 4) * 2 + h, 32)],
                    r3.at[t, (z % 4) * 2 + yh], t, R3, dev(oyl, x, c, zz, h),
                )

    def scatter_low(t):
        for a in range(2):
            zz = (flip(z, 2) // 2) * 2 + (z + a) % 2
            for h in range(2):
                send(
                    proj.at[t, 2, rows((zz % 2) * 2 + h, 64)],
                    r2.at[t, (z % 2) * 2 + yh], t, R2, dev(oyl, x, c, zz, h),
                )
        for h in range(2):
            send(
                proj.at[t, 1, pl.ds(h * 128, 128)], r1.at[t, yh],
                t, R1, dev(oyl, x, c, flip(z, 1), h),
            )
        for h in range(2):
            send(proj.at[t, 0, pl.ds(h * 128, 128)], r0.at[t, yh], t, R0, dev(oyl, x, c, z, h))

    def own_plane(t):
        wait(p1.at[t], recv_sem.at[t, P1])
        qp[t, 0] = add([p1[t, i, 0] for i in range(8)]).astype(BF16)
        qp[t, 1] = add([p1[t, i, 0] for i in range(8, 16)]).astype(BF16)
        qp[t, 2] = add([p1[t, i, 1] for i in range(16)]).astype(BF16)

        def line(i, carry):
            dz = far_first(i)
            zz = (z + dz) % 8
            send(qp.at[t, pl.ds(0, 2)], w6.at[t, dz - 1], t, P6, dev(yl, x, c, zz, yh))
            send(qp.at[t, 2], w7.at[t, dz], t, P7, dev(oyl, x, c, zz, yh))
            return carry

        lax.fori_loop(0, 7, line, 0)
        send(qp.at[t, 2], w7.at[t, 0], t, P7, dev(oyl, x, c, z, yh))

    def own_line(t):
        wait(w6.at[t], recv_sem.at[t, P6])
        for j in range(2):
            tp[t, 1 - j, 0] = add([qp[t, j]] + [w6[t, i, j] for i in range(7)]).astype(BF16)
        wait(w7.at[t], recv_sem.at[t, P7])
        top = add([w7[t, i] for i in range(8)]).astype(BF16)
        tp[t, 0, 1] = top
        tp[t, 1, 1] = top

        def across(i, carry):
            xx = (x + 2 + i) % 4
            for cc in range(2):
                for h in range(2):
                    send(
                        tp.at[t, xx // 2], sib.at[t, pl.ds(6, 2), rows(plane, 16)],
                        t, S67, dev(oyl, xx, cc, z, h),
                    )
            return carry

        lax.fori_loop(0, 4, across, 0)

    def own_ring(t):
        wait(rh.at[t], recv_sem.at[t, RH])
        for k in range(2):
            q45[t, k] = add([rh[t, i, k] for i in range(16)])
        send(q45.at[t], d5.at[t], t, D5, dev(yl, x, 1 - c, z, yh))

    def own_pair(t):
        wait(d5.at[t], recv_sem.at[t, D5])
        t5[t] = (q45[t, 1] + d5[t, 1]).astype(BF16)
        t4[t] = d5[t, 0].astype(BF16)

        @pl.when(yh == c)
        def _():
            def ring(i, carry):
                zz = (z + far_first(i)) % 8
                for h in range(2):
                    send(
                        t5.at[t], sib.at[t, 5, rows(yh * 8 + z, 16)],
                        t, S5, dev(oyl, flip(x, 1), c, zz, h),
                    )
                return carry

            lax.fori_loop(0, 8, ring, 0)

        def ring(i, carry):
            zz = (z + far_first(i)) % 8
            for h in range(2):
                send(t4.at[t], sib.at[t, 4, rows(yh * 8 + z, 16)], t, S4, dev(oyl, x, c, zz, h))
            return carry

        lax.fori_loop(0, 8, ring, 0)

    def pass_on(t):
        half = sib.at[t, 5, rows(c, 128)]
        wait(half, recv_sem.at[t, S5])
        send(half, half, t, F5, dev(yl, x, 1 - c, z, yh))

    def other_half(t):
        wait(sib.at[t, 5, rows(1 - c, 128)], recv_sem.at[t, F5])

    def own_0(t):
        wait(r0.at[t], recv_sem.at[t, R0])
        for h in range(2):
            send(r0.at[t, 1 - h], sib.at[t, 0, rows(yh, 128)], t, S0, dev(oyl, x, c, z, h))

    def own_1(t):
        wait(r1.at[t], recv_sem.at[t, R1])
        q1[t] = add([r1[t, 0], r1[t, 1]]).astype(BF16)
        for h in range(2):
            send(q1.at[t], sib.at[t, 1, rows(yh, 128)], t, S1, dev(oyl, x, c, z, h))

    def own_2(t):
        wait(r2.at[t], recv_sem.at[t, R2])
        q2[t] = add([r2[t, i] for i in range(4)]).astype(BF16)
        for a in range(2):
            zz = (z // 2) * 2 + (z + 1 + a) % 2
            for h in range(2):
                send(q2.at[t], sib.at[t, 2, rows((z % 2) * 2 + yh, 64)], t, S2, dev(oyl, x, c, zz, h))

    def own_3(t):
        wait(r3.at[t], recv_sem.at[t, R3])
        q3[t] = add([r3[t, i] for i in range(8)]).astype(BF16)
        for a in range(4):
            zz = (z // 4) * 4 + (z + 2 + a) % 4
            for h in range(2):
                send(q3.at[t], sib.at[t, 3, rows((z % 4) * 2 + yh, 32)], t, S3, dev(oyl, x, c, zz, h))

    def arrive(t, groups):
        for k, count, s in groups:
            ref = sib.at[t, k] if count == 1 else sib.at[t, pl.ds(k, count)]
            wait(ref, recv_sem.at[t, s])

    def turn(t, levels):
        for k in levels:
            st[k * RANK:(k + 1) * RANK, :] = sib[t, k].T

    LOW = ((0, 1, S0), (1, 1, S1), (2, 1, S2), (3, 1, S3))

    def gram_block(i):
        contract(b_v, pl.ds(i * 256, 256), gacc)
        gram[pl.ds(i * 256, 256), :] = (GAIN * gacc[...]).astype(BF16)

    def through_gram(pair, first=0, last=LEVELS):
        both = jnp.concatenate([sib[0, 2 * pair], sib[0, 2 * pair + 1]], axis=1)
        cols = slice(first * RANK, last * RANK)
        pacc[:, cols] -= jnp.dot(
            both, gram[pl.ds(pair * 256, 256), cols], preferred_element_type=F32
        )

    wait(r_v, in_sem.at[0])
    d_v[...] = (r_v[...].astype(F32) / CENTRE).astype(BF16)

    def project(side):
        cols = pl.ds((1 - side) * HIGH, HIGH)
        for k in range(NCH):
            part = pl.ds(k * CH, CH)
            wait(b_v.at[part, cols], in_sem.at[1 + side * NCH + k])
            p = lax.dot_general(
                d_v[part, :], b_v[part, cols], (((0,), (0,)), ((), ())),
                preferred_element_type=F32,
            )
            pacc[:, cols] = p if k == 0 else pacc[:, cols] + p

    project(0)
    convert(0, (7, 6, 5, 4))
    pl.semaphore_wait(barrier, PEERS)
    scatter_67(0)
    scatter_45(0)
    project(1)
    convert(0, (3, 2, 1, 0))
    scatter_3(0)
    scatter_low(0)
    for k in range(NCH):
        part = pl.ds(k * CH, CH)
        wait(l_v.at[part], in_sem.at[1 + 2 * NCH + k])

    def leaf_0(k, carry):
        part = rows(k, BIG)
        first = r_v[part, :].astype(F32)
        rest = first - jnp.dot(l_v[part, :], d_v[...], preferred_element_type=F32)
        acc_v[part, :] = rest
        u_v[part, :] = (KEEP * (first / CENTRE) + GAIN * rest).astype(BF16)
        return carry

    lax.fori_loop(0, NBIG, leaf_0, 0)
    contract(u_v, slice(None), pacc)
    gram_block(0)
    own_plane(0)
    own_ring(0)
    own_pair(0)
    own_3(0)
    own_2(0)
    own_1(0)
    own_0(0)
    gram_block(1)
    own_line(0)
    gram_block(2)
    gram_block(3)
    pass_on(0)
    arrive(0, LOW)
    through_gram(0)
    through_gram(1)
    arrive(0, ((4, 1, S4),))
    other_half(0)
    through_gram(2)
    arrive(0, ((6, 2, S67),))
    through_gram(3, 6, 8)
    convert(1, (6, 7))
    scatter_67(1)
    through_gram(3, 4, 6)
    convert(1, (4, 5))
    scatter_45(1)
    through_gram(3, 0, 4)
    convert(1, (3, 2, 1, 0))
    scatter_3(1)
    scatter_low(1)

    turn(0, range(LEVELS))

    def middle(k, carry):
        part = rows(k, BIG)
        rest = acc_v[part, :] - jnp.dot(b_v[part, :], st[...], preferred_element_type=F32)
        d0 = r_v[part, :].astype(F32) / CENTRE
        d1 = KEEP * d0 + GAIN * rest
        acc_v[part, :] = rest
        x_v[part, :] = d0 + d1
        d_v[part, :] = d1.astype(BF16)
        return carry

    lax.fori_loop(0, NBIG, middle, 0)

    def leaf_1(k, carry):
        part = rows(k, BIG)
        acc_v[part, :] -= jnp.dot(l_v[part, :], d_v[...], preferred_element_type=F32)
        return carry

    lax.fori_loop(0, NBIG, leaf_1, 0)
    own_plane(1)
    own_ring(1)
    own_pair(1)
    own_3(1)
    own_2(1)
    own_1(1)
    own_0(1)
    own_line(1)
    pass_on(1)
    arrive(1, LOW)
    turn(1, range(4))

    def expand_low(k, carry):
        part = rows(k, BIG)
        acc_v[part, :] -= jnp.dot(
            b_v[part, 0:HIGH], st[0:HIGH, :], preferred_element_type=F32
        )
        return carry

    lax.fori_loop(0, NBIG, expand_low, 0)

    for t in range(ITERS):
        for k, s in ((0, S0), (0, R0), (1, R1), (2, R2), (3, R3), (1, S1), (2, S2), (3, S3), (4, S4)):
            wait(proj.at[t, k], send_sem.at[t, s])

        @pl.when(yh == c)
        def _():
            wait(proj.at[t, 5], send_sem.at[t, S5])

        wait(r0.at[t, 0], send_sem.at[t, F5])
        wait(proj.at[t, pl.ds(4, 2)], send_sem.at[t, RH])
        wait(proj.at[t, pl.ds(6, 2)], send_sem.at[t, P1])
        wait(proj.at[t, pl.ds(6, 2)], send_sem.at[t, S67])
        wait(w6.at[t], send_sem.at[t, P6])
        wait(w7.at[t], send_sem.at[t, P7])
        wait(d5.at[t], send_sem.at[t, D5])
    arrive(1, ((4, 1, S4),))
    other_half(1)
    turn(1, (4, 5))
    arrive(1, ((6, 2, S67),))
    turn(1, (6, 7))


def finish(acc_v, x_v, b_v, st, x_hbm, o_hbm, o_v, sem):
    copies = [pltpu.make_async_copy(x_v, x_hbm, sem.at[0])]
    copies[0].start()
    for k in range(NCH):
        part = pl.ds(k * CH, CH)
        o_v[part, :] = acc_v[part, :] - jnp.dot(
            b_v[part, HIGH:], st[HIGH:, :], preferred_element_type=F32
        )
        copies.append(pltpu.make_async_copy(o_v.at[part], o_hbm.at[part], sem.at[1 + k]))
        copies[-1].start()
    for copy in copies:
        copy.wait()


def on_device(right_side, leaf_blocks, level_bases):
    hbm = pl.BlockSpec(memory_space=pltpu.HBM)
    vmem = pl.BlockSpec(memory_space=pltpu.VMEM)
    field = jax.ShapeDtypeStruct((LEAF, VECS), F32)
    state = pl.pallas_call(
        kernel,
        out_shape=(
            field, field, jax.ShapeDtypeStruct((LEAF, COLS), BF16),
            jax.ShapeDtypeStruct((COLS, VECS), BF16),
        ),
        in_specs=[hbm] * 3,
        out_specs=(vmem,) * 4,
        scratch_shapes=[
            pltpu.VMEM((LEAF, VECS), BF16),
            pltpu.VMEM((LEAF, LEAF), BF16),
            pltpu.VMEM((LEAF, VECS), BF16),
            pltpu.VMEM((LEAF, VECS), BF16),
            pltpu.VMEM((VECS, COLS), F32),
            pltpu.VMEM((VECS, COLS), F32),
            pltpu.VMEM((COLS, COLS), BF16),
            pltpu.VMEM((ITERS, LEVELS, VECS, RANK), BF16),
            pltpu.VMEM((ITERS, LEVELS, VECS, RANK), BF16),
            pltpu.VMEM((ITERS, 2, 128, RANK), BF16),
            pltpu.VMEM((ITERS, 2, 128, RANK), BF16),
            pltpu.VMEM((ITERS, 4, 64, RANK), BF16),
            pltpu.VMEM((ITERS, 8, 32, RANK), BF16),
            pltpu.VMEM((ITERS, 16, 2, 16, RANK), BF16),
            pltpu.VMEM((ITERS, 2, 16, RANK), F32),
            pltpu.VMEM((ITERS, 16, 2, 16, RANK), BF16),
            pltpu.VMEM((ITERS, 7, 2, 16, RANK), BF16),
            pltpu.VMEM((ITERS, 8, 16, RANK), BF16),
            pltpu.VMEM((ITERS, 128, RANK), BF16),
            pltpu.VMEM((ITERS, 64, RANK), BF16),
            pltpu.VMEM((ITERS, 32, RANK), BF16),
            pltpu.VMEM((ITERS, 2, 16, RANK), F32),
            pltpu.VMEM((ITERS, 16, RANK), BF16),
            pltpu.VMEM((ITERS, 16, RANK), BF16),
            pltpu.VMEM((ITERS, 3, 16, RANK), BF16),
            pltpu.VMEM((ITERS, 2, 2, 16, RANK), BF16),
            pltpu.SemaphoreType.DMA((1 + 3 * NCH,)),
            pltpu.SemaphoreType.DMA((ITERS, 17)),
            pltpu.SemaphoreType.DMA((ITERS, 17)),
        ],
        compiler_params=pltpu.CompilerParams(
            collective_id=0, has_side_effects=True, vmem_limit_bytes=40 * 1024 * 1024
        ),
        name="chebyshev",
    )(*(pltpu.with_memory_space_constraint(v, pltpu.HBM) for v in (right_side, leaf_blocks, level_bases)))
    return pl.pallas_call(
        finish,
        out_shape=(field, field),
        in_specs=[vmem] * 4,
        out_specs=(hbm, hbm),
        scratch_shapes=[
            pltpu.VMEM((LEAF, VECS), F32),
            pltpu.SemaphoreType.DMA((1 + NCH,)),
        ],
        compiler_params=pltpu.CompilerParams(vmem_limit_bytes=16 * 1024 * 1024),
        name="finish",
    )(*state)


def solution(mesh):
    return jax.shard_map(
        on_device,
        mesh=mesh,
        in_specs=(P(("wide", "narrow"), None),) * 3,
        out_specs=(P(("wide", "narrow"), None),) * 2,
        check_vma=False,
    )
```
